32 devices in a mesh: leaf: 8 (over z, y), sub: 4 (over x, core).
Axes of the slice: x: 2, y: 2, z: 4, core: 2. Of those that a mesh axis runs over, the one named last changes fastest.
Arguments:
- vectors: bfloat16 [64, 8192], P('sub', 'leaf'), may hold values from -6 to 6
- near_blocks: bfloat16 [32, 9, 256, 256], P(('leaf', 'sub')), may hold values from -0.125 to 0.125
- near_cols: int32 [32, 9], P(('leaf', 'sub')), may hold values from 0 to 31, as said below
- near_mask: int32 [32, 9], P(('leaf', 'sub')), may hold values from 0 to 1, as said below
- leaf_basis: bfloat16 [32, 32, 256], P('leaf'), may hold values from -0.375 to 0.375
- transfer: bfloat16 [48, 32, 32], P('leaf'), may hold values from -1 to 1
- coupling: bfloat16 [56, 27, 32, 32], P('leaf'), may hold values from -0.3125 to 0.3125
- far_targets: int32 [56, 27], P('leaf'), may hold values from 0 to 55, as said below
- far_mask: int32 [56, 27], P('leaf'), may hold values from 0 to 1
Outputs:
- result: bfloat16 [64, 8192], P('sub', 'leaf')
The draws below stay inside these ranges and needn't reach their ends.
Inputs may be any that keep to these rules, and one draw needn't show every extreme that they name: `near_cols`: row i names 9 leaves; its first entry is leaf i; every entry is a leaf of the subtree of leaf i or of the subtree just before or after it; the entries marked live are distinct. `near_mask`: the first entry of each row is 1. `far_targets`: entry (c, k) names a cluster on the same level as cluster c, in any subtree. The 189 entries of one subtree's rows, masked ones included, name clusters of any one subtree at most 32 times; in every draw some subtree is named exactly 32 times, by live entries, from every subtree.
All inputs are finite; a program needn't handle non-finite values.
Results may differ from the reference program's by a relative error of at most 0.0065.
Values may be sent and summed in bfloat16 or wider, within the bound.
A program may use at most 64 MiB of HBM per device.

```python
import jax
import jax.numpy as jnp
from jax import lax

LEAF = 256
RANK = 32
VECS = 64
NEAR = 9
FAR = 27
SUBTREE = 4
CLUSTERS = 7
LEAVES = 32
POINTS = 8192
NODES = 56
SPAN = 8
CAP = 32
N_LEAF = 8


def near_lists(key):
    leaf_ids = jnp.arange(LEAVES, dtype=jnp.int32)
    width_all = 3 * SUBTREE
    position = jnp.arange(width_all, dtype=jnp.int32)
    scores = jax.random.randint(jax.random.fold_in(key, 11), (LEAVES, width_all), 0, 65536, dtype=jnp.int32)
    scores = scores * width_all + position[None, :]
    own_place = leaf_ids % SUBTREE + SUBTREE
    scores = jnp.where(position[None, :] == own_place[:, None], -1, scores)
    best_scores, chosen = lax.top_k(scores, NEAR - 1)
    window_first = (leaf_ids // SUBTREE - 1) * SUBTREE
    columns = window_first[:, None] + chosen.astype(jnp.int32)
    inside = (columns >= 0) & (columns < LEAVES)
    density = jax.random.randint(jax.random.fold_in(key, 12), (LEAVES, 1), 1, 5, dtype=jnp.int32)
    alive = (jax.random.randint(jax.random.fold_in(key, 13), (LEAVES, NEAR - 1), 0, 4, dtype=jnp.int32) < density) & inside
    columns = jnp.where(inside, columns, leaf_ids[:, None])
    columns = jnp.concatenate([leaf_ids[:, None], columns], axis=1).astype(jnp.int32)
    alive = jnp.concatenate([jnp.ones((LEAVES, 1), jnp.int32), alive.astype(jnp.int32)], axis=1)
    return (columns, alive)


def far_lists(key):
    pairs = CLUSTERS * FAR
    slots = SPAN * CAP
    half_span = SPAN // 2
    busiest = jax.random.randint(jax.random.fold_in(key, 21), (), 0, N_LEAF, dtype=jnp.int32)
    tree_ids = jnp.arange(N_LEAF, dtype=jnp.int32)
    slot_ids = jnp.arange(slots, dtype=jnp.int32)
    scores = jax.random.randint(jax.random.fold_in(key, 22), (N_LEAF, slots), 0, 65536, dtype=jnp.int32)
    scores = scores * slots + slot_ids[None, :]
    busy_offset = (busiest - tree_ids + half_span) % N_LEAF
    forced = slot_ids[None, :] // CAP == busy_offset[:, None]
    scores = jnp.where(forced, scores + 1073741824, scores)
    best_scores, chosen = lax.top_k(scores, pairs)
    order_keys = jax.random.split(jax.random.fold_in(key, 23), N_LEAF)
    orders = jax.vmap(lambda single: jax.random.permutation(single, pairs))(order_keys)
    assigned = jnp.take_along_axis(chosen.astype(jnp.int32), orders.astype(jnp.int32), axis=1)
    owners = (tree_ids[:, None] + assigned // CAP - half_span) % N_LEAF
    source_local = jnp.arange(pairs, dtype=jnp.int32) // FAR
    level_first = jnp.zeros((pairs,), jnp.int32)
    level_width = jnp.ones((pairs,), jnp.int32)
    level_start = 0
    level_size = SUBTREE
    while level_size >= 1:
        within = (source_local >= level_start) & (source_local < level_start + level_size)
        level_first = jnp.where(within, level_start, level_first)
        level_width = jnp.where(within, level_size, level_width)
        level_start = level_start + level_size
        level_size = level_size // 2
    picked = jax.random.randint(jax.random.fold_in(key, 24), (N_LEAF, pairs), 0, 1048576, dtype=jnp.int32) % level_width[None, :]
    targets = owners * CLUSTERS + level_first[None, :] + picked
    alive = (jax.random.randint(jax.random.fold_in(key, 25), (N_LEAF, pairs), 0, 4, dtype=jnp.int32) < 3) | (owners == busiest)
    return (targets.reshape(NODES, FAR).astype(jnp.int32), alive.astype(jnp.int32).reshape(NODES, FAR))


def draw_near_cols(key, part):
    return near_lists(key)[0]


def draw_near_mask(key, part):
    return near_lists(key)[1]


def draw_far_targets(key, part):
    return far_lists(key)[0]


def draw_far_mask(key, part):
    return far_lists(key)[1]


def levels(key, extent, shards, least, high):
    gain = 1.0
    for axis_at, parts in shards:
        steps = jax.random.uniform(jax.random.fold_in(jax.random.fold_in(key, 6), axis_at), (parts,), jnp.float32, least / len(shards), high / len(shards))
        gain = gain * jnp.repeat(jnp.exp(steps), extent[axis_at] // parts).reshape((-1,) + (1,) * (len(extent) - 1 - axis_at))
    return gain


def centred(key, shape, deviation, bound, cuts=(), kind=jnp.bfloat16):
    entries = jax.random.normal(key, shape, jnp.float32) * deviation
    if len(cuts) > 0:
        entries = levels(key, shape, cuts, -0.22, 0.18) * entries
    return jnp.clip(entries, min=-bound, max=bound).astype(kind)


def setup_inputs(seed: int = 0) -> dict:
    key_list = jax.random.split(jax.random.key(seed), 10)
    return {
        "vectors": centred(key_list[0], (VECS, POINTS), 1.0, 6.0, ((0, 4), (1, 8))),
        "near_blocks": centred(key_list[1], (LEAVES, NEAR, LEAF, LEAF), (LEAF * NEAR) ** -0.5, 0.125, ((0, 32),)),
        "near_cols": draw_near_cols(jax.random.fold_in(key_list[9], 71), 0),
        "near_mask": draw_near_mask(jax.random.fold_in(key_list[9], 71), 0),
        "leaf_basis": centred(key_list[4], (LEAVES, RANK, LEAF), LEAF ** -0.5, 0.375, ((0, 8),)),
        "transfer": centred(key_list[5], (N_LEAF * (CLUSTERS - 1), RANK, RANK), RANK ** -0.5, 1.0, ((0, 8),)),
        "coupling": centred(key_list[6], (NODES, FAR, RANK, RANK), (RANK * FAR // 2) ** -0.5, 0.3125, ((0, 8),)),
        "far_targets": draw_far_targets(jax.random.fold_in(key_list[9], 71), 0),
        "far_mask": draw_far_mask(jax.random.fold_in(key_list[9], 71), 0),
    }


def level_list():
    sizes_all = []
    level_size = SUBTREE
    while level_size >= 1:
        sizes_all.append(level_size)
        level_size = level_size // 2
    return sizes_all


def reference(vectors, near_blocks, near_cols, near_mask, leaf_basis, transfer, coupling, far_targets, far_mask):
    highest = lax.Precision.HIGHEST
    pieces = vectors.reshape(VECS, LEAVES, LEAF)

    def one_leaf(items):
        blocks, columns, alive = items
        taken = jnp.take(pieces, columns, axis=1).astype(jnp.float32)
        taken = taken * alive.astype(jnp.float32)[None, :, None]
        return jnp.einsum("vkp,kpq->vq", taken, blocks.astype(jnp.float32), precision=highest)

    near = lax.map(one_leaf, (near_blocks, near_cols, near_mask))
    near = jnp.transpose(near, (1, 0, 2)).reshape(VECS, POINTS)

    sizes_all = level_list()
    starts_all = [sum(sizes_all[:number]) for number in range(len(sizes_all))]
    coeffs = jnp.einsum("vnp,nrp->nvr", pieces.astype(jnp.float32), leaf_basis.astype(jnp.float32), precision=highest)
    coeffs = coeffs.reshape(N_LEAF, SUBTREE, VECS, RANK)
    maps_all = transfer.astype(jnp.float32).reshape(N_LEAF, CLUSTERS - 1, RANK, RANK)
    hats = [coeffs]
    for level_no in range(len(sizes_all) - 1):
        level_size = sizes_all[level_no]
        level_start = starts_all[level_no]
        child = hats[-1].reshape(N_LEAF, level_size // 2, 2, VECS, RANK)
        level_maps = maps_all[:, level_start:level_start + level_size].reshape(N_LEAF, level_size // 2, 2, RANK, RANK)
        hats.append(jnp.einsum("npcvr,npcrq->npvq", child, level_maps, precision=highest))
    all_hats = jnp.concatenate(hats, axis=1).reshape(NODES, VECS, RANK)
    terms = jnp.einsum("nvr,nkrq->nkvq", all_hats, coupling.astype(jnp.float32), precision=highest)
    terms = terms * far_mask.astype(jnp.float32)[:, :, None, None]
    incoming = jax.ops.segment_sum(terms.reshape(NODES * FAR, VECS, RANK), far_targets.reshape(-1), num_segments=NODES)
    incoming = incoming.reshape(N_LEAF, CLUSTERS, VECS, RANK)
    downward = [incoming[:, starts_all[number]:starts_all[number] + sizes_all[number]] for number in range(len(sizes_all))]
    for level_no in range(len(sizes_all) - 2, -1, -1):
        level_size = sizes_all[level_no]
        level_start = starts_all[level_no]
        level_maps = maps_all[:, level_start:level_start + level_size].reshape(N_LEAF, level_size // 2, 2, RANK, RANK)
        pushed = jnp.einsum("npvq,npcrq->npcvr", downward[level_no + 1], level_maps, precision=highest)
        downward[level_no] = downward[level_no] + pushed.reshape(N_LEAF, level_size, VECS, RANK)
    basis_tree = leaf_basis.astype(jnp.float32).reshape(N_LEAF, SUBTREE, RANK, LEAF)
    far = jnp.einsum("nsvr,nsrp->vnsp", downward[0], basis_tree, precision=highest).reshape(VECS, POINTS)
    return (near + far).astype(jnp.bfloat16)
```

```python
import functools

import jax
import jax.numpy as jnp
from jax import lax
from jax.experimental import pallas as pl
from jax.experimental.pallas import tpu as pltpu
from jax.sharding import PartitionSpec as P

F32 = jnp.float32
BF16 = jnp.bfloat16
MESH = pl.DeviceIdType.MESH


def mm(a, b):
    return lax.dot_general(a, b, (((1,), (0,)), ((), ())), preferred_element_type=F32)


def nt(a, b):
    return lax.dot_general(a, b, (((1,), (1,)), ((), ())), preferred_element_type=F32)


def iota(shape, dim):
    return lax.broadcasted_iota(jnp.int32, shape, dim)


def quo(x, n):
    if n & (n - 1) == 0:
        return lax.shift_right_logical(x, jnp.int32(n.bit_length() - 1))
    return lax.div(x, jnp.int32(n))


def same(a, b):
    return jnp.where(a == b, 1.0, 0.0).astype(BF16)


def levels_of(subtree):
    found = []
    start = 0
    size = subtree
    while size >= 1:
        found.append((start, size))
        start += size
        size //= 2
    return found


def kernel(
    dims,
    vec_hbm,
    nb_hbm,
    cols_ref,
    live_ref,
    basis_hbm,
    trans_hbm,
    coup_hbm,
    tgt_hbm,
    fmask_hbm,
    out_ref,
    win,
    nb,
    basis,
    trans,
    coup,
    tgt,
    fmask,
    rmat,
    fsend,
    frecv,
    nsend,
    nrecv,
    ld_sem,
    w_send,
    w_recv,
    h_send,
    f_send,
    f_recv,
    n_send,
    n_recv,
):
    trees, subs, pair, chunk = dims
    groups = subs // pair
    own, subtree, leaf = vec_hbm.shape[0], basis.shape[0], basis.shape[2]
    clusters, far, rank = coup.shape[0], coup.shape[1], coup.shape[2]
    near = nb.shape[0]
    levels = levels_of(subtree)
    tree = lax.axis_index("leaf")
    sub = lax.axis_index("sub")
    group, core = lax.div(sub, jnp.int32(pair)), lax.rem(sub, jnp.int32(pair))
    has = (tree > 0, None, tree < trees - 1)
    goes = (tree < trees - 1, None, tree > 0)

    def guarded(cond, action):
        if cond is None:
            action()
        else:
            pl.when(cond)(action)

    loads = [
        pltpu.make_async_copy(vec_hbm, win.at[1, sub], ld_sem.at[0]),
        pltpu.make_async_copy(basis_hbm, basis, ld_sem.at[1]),
        pltpu.make_async_copy(trans_hbm, trans, ld_sem.at[2]),
        pltpu.make_async_copy(tgt_hbm, tgt, ld_sem.at[3]),
        pltpu.make_async_copy(fmask_hbm, fmask, ld_sem.at[4]),
        pltpu.make_async_copy(coup_hbm, coup, ld_sem.at[5]),
        pltpu.make_async_copy(nb_hbm.at[0], nb, ld_sem.at[6]),
    ]
    for load in loads:
        load.start()

    barrier = pltpu.get_barrier_semaphore()

    def greet(to_tree, to_sub):
        pl.semaphore_signal(barrier, inc=1, device_id=(to_tree, to_sub), device_id_type=MESH)

    def other(step):
        return lax.rem(group + step, jnp.int32(groups)) * pair + core

    def greet_tree(step, carry):
        greet(lax.rem(tree + step, jnp.int32(trees)), sub)
        return carry

    lax.fori_loop(1, trees, greet_tree, 0, unroll=trees <= 16)
    for step in range(1, subs):
        greet(tree, lax.rem(sub + step, jnp.int32(subs)))
    for slot in (0, 2):
        for step in range(1, groups):
            guarded(
                goes[slot],
                functools.partial(lambda sl, st: greet(tree + 1 - sl, other(st)), slot, step),
            )
    greeted = (trees - 1) + (subs - 1)
    sides = goes[0].astype(jnp.int32) + goes[2].astype(jnp.int32)

    for slot in (0, 2):
        @pl.when(jnp.logical_not(has[slot]))
        def _():
            win[slot] = jnp.zeros(win.shape[1:], win.dtype)

    loads[0].wait()
    pl.semaphore_wait(barrier, greeted + (groups - 1) * sides)

    def spread(slot, step):
        return pltpu.make_async_remote_copy(
            src_ref=win.at[1, sub],
            dst_ref=win.at[slot, sub],
            send_sem=w_send.at[slot, step],
            recv_sem=w_recv.at[slot, sub],
            device_id=(tree + 1 - slot, other(step)),
            device_id_type=MESH,
        )

    def arrived(slot, from_sub):
        pltpu.make_async_remote_copy(
            src_ref=win.at[slot, from_sub],
            dst_ref=win.at[slot, from_sub],
            send_sem=w_send.at[slot, 0],
            recv_sem=w_recv.at[slot, from_sub],
            device_id=(tree, sub),
            device_id_type=MESH,
        ).wait_recv()

    def hand_over(slot, step, core_step):
        held = other(step)
        return pltpu.make_async_remote_copy(
            src_ref=win.at[slot, held],
            dst_ref=win.at[slot, held],
            send_sem=h_send.at[slot, step, core_step],
            recv_sem=w_recv.at[slot, held],
            device_id=(tree, group * pair + lax.rem(core + core_step, jnp.int32(pair))),
            device_id_type=MESH,
        )

    first_hops = [(slot, step) for step in range(groups) for slot in (0, 2, 1) if (slot, step) != (1, 0)]
    for slot, step in first_hops:
        guarded(goes[slot], functools.partial(lambda a, b: spread(a, b).start(), slot, step))
    for core_step in range(1, pair):
        hand_over(1, 0, core_step).start()

    for load in loads[1:6]:
        load.wait()
    ups = []
    for s in range(subtree):
        piece = win[1, sub, :, s * leaf : (s + 1) * leaf]
        ups.append(nt(piece, basis[s]).astype(BF16))
    for number in range(len(levels) - 1):
        start, size = levels[number]
        for parent in range(size // 2):
            kid = start + 2 * parent
            ups.append((mm(ups[kid], trans[kid]) + mm(ups[kid + 1], trans[kid + 1])).astype(BF16))

    wide = far * rank
    targets = tgt[...]
    owner = jnp.floor((targets.astype(F32) + 0.5) * (1.0 / clusters)).astype(jnp.int32)
    place = targets - owner * clusters
    owner = jnp.where(fmask[...] > 0, owner, -1)
    spread_k = same(quo(iota((far, wide), 1), rank), iota((far, wide), 0))
    spread_rows = same(quo(iota((wide, far), 0), rank), iota((wide, far), 1))
    tile_wide = same(iota((rank, wide), 1) & (rank - 1), iota((rank, wide), 0))
    for start, size in levels:
        width = size * rank
        tile = same(iota((rank, width), 1) & (rank - 1), iota((rank, width), 0))
        for c in range(start, start + size):
            tiled = mm(coup[c].reshape(wide, rank), tile)
            picks = same(quo(iota((width, far), 0), rank) + start, place[c : c + 1, :])
            chosen = nt(spread_rows, picks)
            rmat[c, :, :width] = (tiled * chosen).astype(BF16)
    up_wide = [mm(up, tile_wide) for up in ups]

    def couple(number, carry):
        base = number * chunk
        sums = []
        for start, size in levels:
            total = None
            for c in range(start, start + size):
                mine = same(quo(iota((chunk * own, far), 0), own) + base, owner[c : c + 1, :])
                left = mm(mine, spread_k) * jnp.concatenate([up_wide[c]] * chunk, axis=0)
                term = mm(left.astype(BF16), rmat[c, :, : size * rank])
                total = term if total is None else total + term
            sums.append(total)
        spare = fsend.shape[2] - clusters * rank
        if spare:
            sums.append(jnp.zeros((chunk * own, spare), F32))
        joined = jnp.concatenate(sums, axis=1).astype(BF16)
        fsend[pl.ds(base, chunk)] = joined.reshape(chunk, own, fsend.shape[2])
        return carry

    lax.fori_loop(0, trees // chunk, couple, 0, unroll=trees == chunk)

    def far_copy(step):
        to = lax.rem(tree + step, jnp.int32(trees))
        return pltpu.make_async_remote_copy(
            src_ref=fsend.at[to],
            dst_ref=frecv.at[tree],
            send_sem=f_send.at[to],
            recv_sem=f_recv.at[tree],
            device_id=(to, sub),
            device_id_type=MESH,
        )

    def far_arrived(step):
        source = lax.rem(tree + step, jnp.int32(trees))
        pltpu.make_async_remote_copy(
            src_ref=fsend.at[source],
            dst_ref=frecv.at[source],
            send_sem=f_send.at[source],
            recv_sem=f_recv.at[source],
            device_id=(source, sub),
            device_id_type=MESH,
        ).wait_recv()
        return source

    def start_far(step, carry):
        far_copy(step).start()
        return carry

    lax.fori_loop(1, trees, start_far, 0, unroll=trees <= 16)

    loads[6].wait()
    total = jnp.zeros((subs * own, leaf), F32)

    def relay(slot, step):
        arrived(slot, other(step))
        for core_step in range(1, pair):
            hand_over(slot, step, core_step).start()

    def take(slot, step, core_step):
        from_core = lax.rem(core + core_step, jnp.int32(pair))
        arrived(slot, lax.rem(group + step, jnp.int32(groups)) * pair + from_core)

    for slot, step in [(1, step) for step in range(1, groups)] + [
        (slot, step) for step in range(groups) for slot in (0, 2)
    ]:
        guarded(has[slot], functools.partial(relay, slot, step))

    for slot in (1, 0, 2):
        for step in range(groups):
            for core_step in range(1, pair):
                guarded(has[slot], functools.partial(take, slot, step, core_step))
        for q in range(subtree):
            wanted = (tree + slot - 1) * subtree + q
            index = jnp.int32(0)
            alive = jnp.int32(0)
            for k in range(near):
                hit = jnp.where(cols_ref[0, k] == wanted, live_ref[0, k], 0)
                index = index + hit * k
                alive = alive + hit
            piece = win[slot, :, :, q * leaf : (q + 1) * leaf].reshape(subs * own, leaf)
            total = total + mm(piece, nb[index]) * alive.astype(F32)

    parts = total.reshape(subs, own, leaf).astype(BF16)
    nsend[...] = parts
    nrecv[sub] = nsend[sub]

    def near_copy(step):
        to = lax.rem(sub + step, jnp.int32(subs))
        return pltpu.make_async_remote_copy(
            src_ref=nsend.at[to],
            dst_ref=nrecv.at[sub],
            send_sem=n_send.at[to],
            recv_sem=n_recv.at[sub],
            device_id=(tree, to),
            device_id_type=MESH,
        )

    def near_arrived(step):
        source = lax.rem(sub + step, jnp.int32(subs))
        pltpu.make_async_remote_copy(
            src_ref=nsend.at[source],
            dst_ref=nrecv.at[source],
            send_sem=n_send.at[source],
            recv_sem=n_recv.at[source],
            device_id=(tree, source),
            device_id_type=MESH,
        ).wait_recv()

    for step in range(1, subs):
        near_copy(step).start()

    def add_far(step, carry):
        return carry + frecv[far_arrived(step)].astype(F32)

    incoming = lax.fori_loop(1, trees, add_far, fsend[tree].astype(F32), unroll=trees <= 16)
    downs = incoming[:, levels[-1][0] * rank : clusters * rank]
    for number in range(len(levels) - 2, -1, -1):
        start, size = levels[number]
        pushed = []
        for parent in range(size // 2):
            maps = trans[start + 2 * parent : start + 2 * parent + 2].reshape(2 * rank, rank)
            pushed.append(nt(downs[:, parent * rank : (parent + 1) * rank].astype(BF16), maps))
        pushed = pushed[0] if len(pushed) == 1 else jnp.concatenate(pushed, axis=1)
        downs = incoming[:, start * rank : (start + size) * rank] + pushed
    fars = [
        mm(downs[:, s * rank : (s + 1) * rank].astype(BF16), basis[s]) for s in range(subtree)
    ]

    for step in range(1, subs):
        near_arrived(step)
    for s in range(subtree):
        out_ref[:, s * leaf : (s + 1) * leaf] = (nrecv[s].astype(F32) + fars[s]).astype(BF16)

    for slot, step in first_hops:
        guarded(goes[slot], functools.partial(lambda a, b: spread(a, b).wait_send(), slot, step))
    for slot in range(3):
        for step in range(groups):
            for core_step in range(1, pair):
                guarded(
                    has[slot],
                    functools.partial(lambda *at: hand_over(*at).wait_send(), slot, step, core_step),
                )

    def end_far(step, carry):
        far_copy(step).wait_send()
        return carry

    lax.fori_loop(1, trees, end_far, 0, unroll=trees <= 16)
    for step in range(1, subs):
        near_copy(step).wait_send()


def local(vectors, near_blocks, near_cols, near_mask, leaf_basis, transfer, coupling, far_targets, far_mask):
    trees, subs = lax.axis_size("leaf"), lax.axis_size("sub")
    pair = 2 if subs % 2 == 0 else 1
    groups = subs // pair
    chunk = 8 if trees % 8 == 0 else trees
    own, points = vectors.shape
    clusters, far, rank = coupling.shape[:3]
    leaf = leaf_basis.shape[2]
    lanes = -(-clusters * rank // 128) * 128
    any_spec = pl.BlockSpec(memory_space=pl.ANY)
    smem = pl.BlockSpec(memory_space=pltpu.SMEM)
    dma = pltpu.SemaphoreType.DMA
    return pl.pallas_call(
        functools.partial(kernel, (trees, subs, pair, chunk)),
        out_shape=jax.ShapeDtypeStruct((own, points), BF16),
        in_specs=[any_spec, any_spec, smem, smem] + [any_spec] * 5,
        out_specs=pl.BlockSpec(memory_space=pltpu.VMEM),
        scratch_shapes=[
            pltpu.VMEM((3, subs, own, points), BF16),
            pltpu.VMEM(near_blocks.shape[1:], BF16),
            pltpu.VMEM(leaf_basis.shape, BF16),
            pltpu.VMEM(transfer.shape, BF16),
            pltpu.VMEM(coupling.shape, BF16),
            pltpu.VMEM(far_targets.shape, jnp.int32),
            pltpu.VMEM(far_mask.shape, jnp.int32),
            pltpu.VMEM((clusters, far * rank, leaf_basis.shape[0] * rank), BF16),
            pltpu.VMEM((trees, own, lanes), BF16),
            pltpu.VMEM((trees, own, lanes), BF16),
            pltpu.VMEM((subs, own, leaf), BF16),
            pltpu.VMEM((subs, own, leaf), BF16),
            dma((7,)),
            dma((3, groups)),
            dma((3, subs)),
            dma((3, groups, pair)),
            dma((trees,)),
            dma((trees,)),
            dma((subs,)),
            dma((subs,)),
        ],
        compiler_params=pltpu.CompilerParams(collective_id=0, has_side_effects=True),
    )(vectors, near_blocks, near_cols, near_mask, leaf_basis, transfer, coupling, far_targets, far_mask)


def solution(mesh):
    return jax.shard_map(
        local,
        mesh=mesh,
        in_specs=(
            P("sub", "leaf"),
            P(("leaf", "sub"), None, None, None),
            P(("leaf", "sub"), None),
            P(("leaf", "sub"), None),
            P("leaf", None, None),
            P("leaf", None, None),
            P("leaf", None, None, None),
            P("leaf", None),
            P("leaf", None),
        ),
        out_specs=P("sub", "leaf"),
        check_vma=False,
    )
```

```python
import functools

import jax
import jax.numpy as jnp
from jax import lax
from jax.experimental import pallas as pl
from jax.experimental.pallas import tpu as pltpu
from jax.sharding import PartitionSpec as P

F32 = jnp.float32
BF16 = jnp.bfloat16
MESH = pl.DeviceIdType.MESH


def mm(a, b):
    return lax.dot_general(a, b, (((1,), (0,)), ((), ())), preferred_element_type=F32)


def nt(a, b):
    return lax.dot_general(a, b, (((1,), (1,)), ((), ())), preferred_element_type=F32)


def iota(shape, dim):
    return lax.broadcasted_iota(jnp.int32, shape, dim)


def quo(x, n):
    if n & (n - 1) == 0:
        return lax.shift_right_logical(x, jnp.int32(n.bit_length() - 1))
    return lax.div(x, jnp.int32(n))


def same(a, b):
    return jnp.where(a == b, 1.0, 0.0).astype(BF16)


def levels_of(subtree):
    found = []
    start = 0
    size = subtree
    while size >= 1:
        found.append((start, size))
        start += size
        size //= 2
    return found


def kernel(
    dims,
    vec_hbm,
    nb_hbm,
    cols_ref,
    live_ref,
    basis_hbm,
    trans_hbm,
    coup_hbm,
    tgt_hbm,
    fmask_hbm,
    out_ref,
    win,
    nb,
    wown,
    wpeer,
    basis,
    trans,
    coup,
    tgt,
    fmask,
    rmat,
    fsend,
    frecv,
    nsend,
    nrecv,
    known,
    ld_sem,
    w_send,
    w_recv,
    h_send,
    h_recv,
    f_send,
    f_recv,
    n_send,
    n_recv,
):
    trees, subs, pair, chunk = dims
    groups = subs // pair
    own, subtree, leaf = vec_hbm.shape[0], basis.shape[0], basis.shape[2]
    clusters, far, rank = coup.shape[0], coup.shape[1], coup.shape[2]
    near = nb.shape[0]
    levels = levels_of(subtree)
    tree = lax.axis_index("leaf")
    sub = lax.axis_index("sub")
    group, core = lax.div(sub, jnp.int32(pair)), lax.rem(sub, jnp.int32(pair))
    has = (tree > 0, None, tree < trees - 1)
    goes = (tree < trees - 1, None, tree > 0)

    def guarded(cond, action):
        if cond is None:
            action()
        else:
            pl.when(cond)(action)

    loads = [
        pltpu.make_async_copy(vec_hbm, win.at[1, group], ld_sem.at[0]),
        pltpu.make_async_copy(basis_hbm, basis, ld_sem.at[1]),
        pltpu.make_async_copy(trans_hbm, trans, ld_sem.at[2]),
        pltpu.make_async_copy(tgt_hbm, tgt, ld_sem.at[3]),
        pltpu.make_async_copy(fmask_hbm, fmask, ld_sem.at[4]),
        pltpu.make_async_copy(coup_hbm, coup, ld_sem.at[5]),
        pltpu.make_async_copy(nb_hbm.at[0], nb, ld_sem.at[6]),
    ]
    for number in (0, 6, 1, 2, 3, 4, 5):
        loads[number].start()

    barrier = pltpu.get_barrier_semaphore()

    def greet(to_tree, to_sub):
        pl.semaphore_signal(barrier, inc=1, device_id=(to_tree, to_sub), device_id_type=MESH)

    def other(step):
        return lax.rem(group + step, jnp.int32(groups)) * pair + core

    half = max(1, trees // 2)

    def both_ways(reach, action):
        for there in (-reach, reach):
            @pl.when((tree + there >= 0) & (tree + there < trees))
            def _():
                action(tree + there)

    def partner(core_step):
        return group * pair + lax.rem(core + core_step, jnp.int32(pair))

    def greet_tree(reach, carry):
        both_ways(reach, lambda to: greet(to, sub))
        return carry

    for slot in (0, 2):
        for step in range(1, groups):
            guarded(
                goes[slot],
                functools.partial(lambda sl, st: greet(tree + 1 - sl, other(st)), slot, step),
            )
    lax.fori_loop(1, half + 1, greet_tree, 0, unroll=half <= 16)
    for step in range(1, groups):
        greet(tree, other(step))
    for core_step in range(1, pair):
        greet(tree, partner(core_step))
    sides = goes[0].astype(jnp.int32) + goes[2].astype(jnp.int32)
    greeted = (pair - 1) + (groups - 1) * (1 + sides)
    greeted = greeted + jnp.minimum(tree, half) + jnp.minimum(trees - 1 - tree, half)

    for slot in (0, 2):
        @pl.when(jnp.logical_not(has[slot]))
        def _():
            win[slot] = jnp.zeros(win.shape[1:], win.dtype)

    loads[6].wait()
    for j in range(3 * subtree):
        wanted = (tree - 1) * subtree + j
        index = jnp.int32(0)
        alive = jnp.int32(0)
        for k in range(near):
            hit = jnp.where(cols_ref[0, k] == wanted, live_ref[0, k], 0)
            index = index + hit * k
            alive = alive + hit
        wown[j] = jnp.where(alive > 0, nb[index], jnp.zeros((leaf, leaf), BF16))

    loads[0].wait()
    pl.semaphore_wait(barrier, greeted)

    def spread(slot, step):
        return pltpu.make_async_remote_copy(
            src_ref=win.at[1, group],
            dst_ref=win.at[slot, group],
            send_sem=w_send.at[slot, step],
            recv_sem=w_recv.at[slot, group],
            device_id=(tree + 1 - slot, other(step)),
            device_id_type=MESH,
        )

    def arrived(slot, step):
        held = lax.rem(group + step, jnp.int32(groups))
        pltpu.make_async_remote_copy(
            src_ref=win.at[slot, held],
            dst_ref=win.at[slot, held],
            send_sem=w_send.at[slot, 0],
            recv_sem=w_recv.at[slot, held],
            device_id=(tree, sub),
            device_id_type=MESH,
        ).wait_recv()

    def swap(core_step):
        return pltpu.make_async_remote_copy(
            src_ref=wown,
            dst_ref=wpeer.at[pair - 1 - core_step],
            send_sem=h_send.at[core_step - 1],
            recv_sem=h_recv.at[pair - 1 - core_step],
            device_id=(tree, partner(core_step)),
            device_id_type=MESH,
        )

    first_hops = [(slot, step) for step in range(groups - 1, -1, -1) for slot in (0, 2, 1) if (slot, step) != (1, 0)]
    for slot, step in first_hops:
        guarded(goes[slot], functools.partial(lambda a, b: spread(a, b).start(), slot, step))
    for core_step in range(1, pair):
        swap(core_step).start()

    both_ways(
        half,
        lambda to: pl.semaphore_signal(known, inc=1, device_id=(to, sub), device_id_type=MESH),
    )

    for load in loads[1:6]:
        load.wait()
    ups = []
    for s in range(subtree):
        piece = win[1, group, :, s * leaf : (s + 1) * leaf]
        ups.append(nt(piece, basis[s]).astype(BF16))
    for number in range(len(levels) - 1):
        start, size = levels[number]
        for parent in range(size // 2):
            kid = start + 2 * parent
            ups.append((mm(ups[kid], trans[kid]) + mm(ups[kid + 1], trans[kid + 1])).astype(BF16))

    wide = far * rank
    targets = tgt[...]
    owner = jnp.floor((targets.astype(F32) + 0.5) * (1.0 / clusters)).astype(jnp.int32)
    place = targets - owner * clusters
    owner = jnp.where(fmask[...] > 0, owner, -1)
    spread_k = same(quo(iota((far, wide), 1), rank), iota((far, wide), 0))
    spread_rows = same(quo(iota((wide, far), 0), rank), iota((wide, far), 1))
    tile_wide = same(iota((rank, wide), 1) & (rank - 1), iota((rank, wide), 0))
    for start, size in levels:
        width = size * rank
        tile = same(iota((rank, width), 1) & (rank - 1), iota((rank, width), 0))
        for c in range(start, start + size):
            tiled = mm(coup[c].reshape(wide, rank), tile)
            picks = same(quo(iota((width, far), 0), rank) + start, place[c : c + 1, :])
            chosen = nt(spread_rows, picks)
            rmat[c, :, :width] = (tiled * chosen).astype(BF16)
    up_wide = [mm(up, tile_wide) for up in ups]

    def couple(number, carry):
        base = number * chunk
        sums = []
        for start, size in levels:
            total = None
            for c in range(start, start + size):
                mine = same(quo(iota((chunk * own, far), 0), own) + base, owner[c : c + 1, :])
                left = mm(mine, spread_k) * jnp.concatenate([up_wide[c]] * chunk, axis=0)
                term = mm(left.astype(BF16), rmat[c, :, : size * rank])
                total = term if total is None else total + term
            sums.append(total)
        spare = fsend.shape[2] - clusters * rank
        if spare:
            sums.append(jnp.zeros((chunk * own, spare), F32))
        joined = jnp.concatenate(sums, axis=1).astype(BF16)
        fsend[pl.ds(base, chunk)] = joined.reshape(chunk, own, fsend.shape[2])
        return carry

    lax.fori_loop(0, trees // chunk, couple, 0, unroll=trees == chunk)

    def far_copy(step):
        to = lax.rem(tree + step, jnp.int32(trees))
        return pltpu.make_async_remote_copy(
            src_ref=fsend.at[to],
            dst_ref=frecv.at[tree],
            send_sem=f_send.at[to],
            recv_sem=f_recv.at[tree],
            device_id=(to, sub),
            device_id_type=MESH,
        )

    def far_arrived(step):
        source = lax.rem(tree + step, jnp.int32(trees))
        pltpu.make_async_remote_copy(
            src_ref=fsend.at[source],
            dst_ref=frecv.at[source],
            send_sem=f_send.at[source],
            recv_sem=f_recv.at[source],
            device_id=(source, sub),
            device_id_type=MESH,
        ).wait_recv()
        return source

    def start_far(step, carry):
        far_copy(step).start()
        return carry

    heard = (tree >= half).astype(jnp.int32) + (tree + half < trees).astype(jnp.int32)
    pl.semaphore_wait(known, heard)
    lax.fori_loop(1, trees, start_far, 0, unroll=trees <= 16)

    rows = groups * own
    totals = [jnp.zeros((rows, leaf), F32)] * pair
    for slot in (1, 0, 2):
        for step in range(groups):
            if (slot, step) != (1, 0):
                guarded(has[slot], functools.partial(arrived, slot, step))
        if slot == 1:
            for core_step in range(1, pair):
                swap(core_step).wait_recv()
        for q in range(subtree):
            piece = win[slot, :, :, q * leaf : (q + 1) * leaf].reshape(rows, leaf)
            for core_step in range(pair):
                blocks = wown if core_step == 0 else wpeer.at[core_step - 1]
                totals[core_step] = totals[core_step] + mm(piece, blocks[slot * subtree + q])

    for core_step in range(pair):
        leaf_core = lax.rem(core + core_step, jnp.int32(pair))
        nsend[:, leaf_core] = totals[core_step].reshape(groups, own, leaf).astype(BF16)
    nrecv[group] = nsend[group]

    def near_copy(step):
        to = lax.rem(group + step, jnp.int32(groups))
        return pltpu.make_async_remote_copy(
            src_ref=nsend.at[to],
            dst_ref=nrecv.at[group],
            send_sem=n_send.at[to],
            recv_sem=n_recv.at[group],
            device_id=(tree, other(step)),
            device_id_type=MESH,
        )

    def near_arrived(step):
        source = lax.rem(group + step, jnp.int32(groups))
        pltpu.make_async_remote_copy(
            src_ref=nsend.at[source],
            dst_ref=nrecv.at[source],
            send_sem=n_send.at[source],
            recv_sem=n_recv.at[source],
            device_id=(tree, other(step)),
            device_id_type=MESH,
        ).wait_recv()

    for step in range(1, groups):
        near_copy(step).start()

    def add_far(step, carry):
        return carry + frecv[far_arrived(step)].astype(F32)

    incoming = lax.fori_loop(1, trees, add_far, fsend[tree].astype(F32), unroll=trees <= 16)
    downs = incoming[:, levels[-1][0] * rank : clusters * rank]
    for number in range(len(levels) - 2, -1, -1):
        start, size = levels[number]
        pushed = []
        for parent in range(size // 2):
            maps = trans[start + 2 * parent : start + 2 * parent + 2].reshape(2 * rank, rank)
            pushed.append(nt(downs[:, parent * rank : (parent + 1) * rank].astype(BF16), maps))
        pushed = pushed[0] if len(pushed) == 1 else jnp.concatenate(pushed, axis=1)
        downs = incoming[:, start * rank : (start + size) * rank] + pushed
    fars = [
        mm(downs[:, s * rank : (s + 1) * rank].astype(BF16), basis[s]) for s in range(subtree)
    ]

    for step in range(1, groups):
        near_arrived(step)
    for s in range(subtree):
        near_part = nrecv[s // pair, s % pair].astype(F32)
        out_ref[:, s * leaf : (s + 1) * leaf] = (near_part + fars[s]).astype(BF16)

    for slot, step in first_hops:
        guarded(goes[slot], functools.partial(lambda a, b: spread(a, b).wait_send(), slot, step))
    for core_step in range(1, pair):
        swap(core_step).wait_send()

    def end_far(step, carry):
        far_copy(step).wait_send()
        return carry

    lax.fori_loop(1, trees, end_far, 0, unroll=trees <= 16)
    for step in range(1, groups):
        near_copy(step).wait_send()


def local(vectors, near_blocks, near_cols, near_mask, leaf_basis, transfer, coupling, far_targets, far_mask):
    trees, subs = lax.axis_size("leaf"), lax.axis_size("sub")
    pair = 2 if subs % 2 == 0 else 1
    groups = subs // pair
    chunk = 8 if trees % 8 == 0 else trees
    own, points = vectors.shape
    clusters, far, rank = coupling.shape[:3]
    leaf = leaf_basis.shape[2]
    window = 3 * leaf_basis.shape[0]
    lanes = -(-clusters * rank // 128) * 128
    any_spec = pl.BlockSpec(memory_space=pl.ANY)
    smem = pl.BlockSpec(memory_space=pltpu.SMEM)
    dma = pltpu.SemaphoreType.DMA
    return pl.pallas_call(
        functools.partial(kernel, (trees, subs, pair, chunk)),
        out_shape=jax.ShapeDtypeStruct((own, points), BF16),
        in_specs=[any_spec, any_spec, smem, smem] + [any_spec] * 5,
        out_specs=pl.BlockSpec(memory_space=pltpu.VMEM),
        scratch_shapes=[
            pltpu.VMEM((3, groups, own, points), BF16),
            pltpu.VMEM(near_blocks.shape[1:], BF16),
            pltpu.VMEM((window, leaf, leaf), BF16),
            pltpu.VMEM((max(1, pair - 1), window, leaf, leaf), BF16),
            pltpu.VMEM(leaf_basis.shape, BF16),
            pltpu.VMEM(transfer.shape, BF16),
            pltpu.VMEM(coupling.shape, BF16),
            pltpu.VMEM(far_targets.shape, jnp.int32),
            pltpu.VMEM(far_mask.shape, jnp.int32),
            pltpu.VMEM((clusters, far * rank, leaf_basis.shape[0] * rank), BF16),
            pltpu.VMEM((trees, own, lanes), BF16),
            pltpu.VMEM((trees, own, lanes), BF16),
            pltpu.VMEM((groups, pair, own, leaf), BF16),
            pltpu.VMEM((groups, pair, own, leaf), BF16),
            pltpu.SemaphoreType.REGULAR,
            dma((7,)),
            dma((3, groups)),
            dma((3, groups)),
            dma((max(1, pair - 1),)),
            dma((max(1, pair - 1),)),
            dma((trees,)),
            dma((trees,)),
            dma((groups,)),
            dma((groups,)),
        ],
        compiler_params=pltpu.CompilerParams(collective_id=0, has_side_effects=True),
    )(vectors, near_blocks, near_cols, near_mask, leaf_basis, transfer, coupling, far_targets, far_mask)


def solution(mesh):
    return jax.shard_map(
        local,
        mesh=mesh,
        in_specs=(
            P("sub", "leaf"),
            P(("leaf", "sub"), None, None, None),
            P(("leaf", "sub"), None),
            P(("leaf", "sub"), None),
            P("leaf", None, None),
            P("leaf", None, None),
            P("leaf", None, None, None),
            P("leaf", None),
            P("leaf", None),
        ),
        out_specs=P("sub", "leaf"),
        check_vma=False,
    )
```

```python
import functools

import jax
import jax.numpy as jnp
from jax import lax
from jax.experimental import pallas as pl
from jax.experimental.pallas import tpu as pltpu
from jax.sharding import PartitionSpec as P

F32 = jnp.float32
BF16 = jnp.bfloat16
MESH = pl.DeviceIdType.MESH


def mm(a, b):
    return lax.dot_general(a, b, (((1,), (0,)), ((), ())), preferred_element_type=F32)


def nt(a, b):
    return lax.dot_general(a, b, (((1,), (1,)), ((), ())), preferred_element_type=F32)


def iota(shape, dim):
    return lax.broadcasted_iota(jnp.int32, shape, dim)


def quo(x, n):
    if n & (n - 1) == 0:
        return lax.shift_right_logical(x, jnp.int32(n.bit_length() - 1))
    return lax.div(x, jnp.int32(n))


def same(a, b):
    return jnp.where(a == b, 1.0, 0.0).astype(BF16)


def levels_of(subtree):
    found = []
    start = 0
    size = subtree
    while size >= 1:
        found.append((start, size))
        start += size
        size //= 2
    return found


def kernel(
    dims,
    vec_hbm,
    nb_hbm,
    cols_ref,
    live_ref,
    basis_hbm,
    trans_hbm,
    coup_hbm,
    tgt_hbm,
    fmask_hbm,
    out_ref,
    win,
    nb,
    wown,
    wpeer,
    basis,
    trans,
    coup,
    tgt,
    fmask,
    dmat,
    rmat,
    fsend,
    frecv,
    nsend,
    nrecv,
    known,
    ld_sem,
    w_send,
    w_recv,
    h_send,
    h_recv,
    f_send,
    f_recv,
    n_send,
    n_recv,
):
    trees, subs, pair, chunk = dims
    groups = subs // pair
    own, subtree, leaf = vec_hbm.shape[0], basis.shape[0], basis.shape[2]
    clusters, far, rank = coup.shape[0], coup.shape[1], coup.shape[2]
    near = nb.shape[0]
    levels = levels_of(subtree)
    tree = lax.axis_index("leaf")
    sub = lax.axis_index("sub")
    group, core = lax.div(sub, jnp.int32(pair)), lax.rem(sub, jnp.int32(pair))
    has = (tree > 0, None, tree < trees - 1)
    goes = (tree < trees - 1, None, tree > 0)

    def guarded(cond, action):
        if cond is None:
            action()
        else:
            pl.when(cond)(action)

    loads = [
        pltpu.make_async_copy(vec_hbm, win.at[1, group], ld_sem.at[0]),
        pltpu.make_async_copy(basis_hbm, basis, ld_sem.at[1]),
        pltpu.make_async_copy(trans_hbm, trans, ld_sem.at[2]),
        pltpu.make_async_copy(tgt_hbm, tgt, ld_sem.at[3]),
        pltpu.make_async_copy(fmask_hbm, fmask, ld_sem.at[4]),
        pltpu.make_async_copy(coup_hbm, coup, ld_sem.at[5]),
        pltpu.make_async_copy(nb_hbm.at[0], nb, ld_sem.at[6]),
    ]
    for number in (0, 6, 1, 2, 3, 4, 5):
        loads[number].start()

    barrier = pltpu.get_barrier_semaphore()

    def greet(to_tree, to_sub):
        pl.semaphore_signal(barrier, inc=1, device_id=(to_tree, to_sub), device_id_type=MESH)

    def other(step):
        return lax.rem(group + step, jnp.int32(groups)) * pair + core

    half = max(1, trees // 2)

    def both_ways(reach, action):
        for there in (-reach, reach):
            @pl.when((tree + there >= 0) & (tree + there < trees))
            def _():
                action(tree + there)

    def partner(core_step):
        return group * pair + lax.rem(core + core_step, jnp.int32(pair))

    def greet_tree(reach, carry):
        both_ways(reach, lambda to: greet(to, sub))
        return carry

    for slot in (0, 2):
        for step in range(1, groups):
            guarded(
                goes[slot],
                functools.partial(lambda sl, st: greet(tree + 1 - sl, other(st)), slot, step),
            )
    lax.fori_loop(1, half + 1, greet_tree, 0, unroll=half <= 16)
    for step in range(1, groups):
        greet(tree, other(step))
    for core_step in range(1, pair):
        greet(tree, partner(core_step))
    sides = goes[0].astype(jnp.int32) + goes[2].astype(jnp.int32)
    greeted = (pair - 1) + (groups - 1) * (1 + sides)
    greeted = greeted + jnp.minimum(tree, half) + jnp.minimum(trees - 1 - tree, half)

    for slot in (0, 2):
        @pl.when(jnp.logical_not(has[slot]))
        def _():
            win[slot] = jnp.zeros(win.shape[1:], win.dtype)

    loads[6].wait()
    for j in range(3 * subtree):
        wanted = (tree - 1) * subtree + j
        index = jnp.int32(0)
        alive = jnp.int32(0)
        for k in range(near):
            hit = jnp.where(cols_ref[0, k] == wanted, live_ref[0, k], 0)
            index = index + hit * k
            alive = alive + hit
        wown[j] = jnp.where(alive > 0, nb[index], jnp.zeros((leaf, leaf), BF16))

    for load in loads[1:3]:
        load.wait()
    dmat[...] = jnp.zeros(dmat.shape, BF16)
    folded = {s: {s: basis[s]} for s in range(subtree)}
    for number in range(len(levels) - 1):
        start, size = levels[number]
        for kid in range(start, start + size):
            parent = start + size + (kid - start) // 2
            for s, block in folded[kid].items():
                raised = lax.dot_general(
                    trans[kid], block, (((0,), (0,)), ((), ())), preferred_element_type=F32
                )
                folded.setdefault(parent, {})[s] = raised.astype(BF16)
    for c, blocks in folded.items():
        for s, block in blocks.items():
            dmat[c * rank : (c + 1) * rank, s * leaf : (s + 1) * leaf] = block
    loads[0].wait()
    pl.semaphore_wait(barrier, greeted)

    def spread(slot, step):
        return pltpu.make_async_remote_copy(
            src_ref=win.at[1, group],
            dst_ref=win.at[slot, group],
            send_sem=w_send.at[slot, step],
            recv_sem=w_recv.at[slot, group],
            device_id=(tree + 1 - slot, other(step)),
            device_id_type=MESH,
        )

    def arrived(slot, step):
        held = lax.rem(group + step, jnp.int32(groups))
        pltpu.make_async_remote_copy(
            src_ref=win.at[slot, held],
            dst_ref=win.at[slot, held],
            send_sem=w_send.at[slot, 0],
            recv_sem=w_recv.at[slot, held],
            device_id=(tree, sub),
            device_id_type=MESH,
        ).wait_recv()

    def swap(core_step, slot):
        part = pl.ds(slot * subtree, subtree)
        return pltpu.make_async_remote_copy(
            src_ref=wown.at[part],
            dst_ref=wpeer.at[pair - 1 - core_step, part],
            send_sem=h_send.at[core_step - 1, slot],
            recv_sem=h_recv.at[pair - 1 - core_step, slot],
            device_id=(tree, partner(core_step)),
            device_id_type=MESH,
        )

    first_hops = [(slot, step) for step in range(groups - 1, -1, -1) for slot in (0, 2, 1) if (slot, step) != (1, 0)]
    for slot, step in first_hops:
        guarded(goes[slot], functools.partial(lambda a, b: spread(a, b).start(), slot, step))
    for core_step in range(1, pair):
        for slot in (1, 0, 2):
            swap(core_step, slot).start()

    both_ways(
        half,
        lambda to: pl.semaphore_signal(known, inc=1, device_id=(to, sub), device_id_type=MESH),
    )

    for load in loads[3:6]:
        load.wait()
    lifted = nt(win[1, group], dmat[...]).astype(BF16)
    ups = [lifted[:, c * rank : (c + 1) * rank] for c in range(clusters)]

    wide = far * rank
    targets = tgt[...]
    owner = jnp.floor((targets.astype(F32) + 0.5) * (1.0 / clusters)).astype(jnp.int32)
    place = targets - owner * clusters
    owner = jnp.where(fmask[...] > 0, owner, -1)
    spread_k = same(quo(iota((far, wide), 1), rank), iota((far, wide), 0))
    spread_rows = same(quo(iota((wide, far), 0), rank), iota((wide, far), 1))
    tile_wide = same(iota((rank, wide), 1) & (rank - 1), iota((rank, wide), 0))
    for start, size in levels:
        width = size * rank
        tile = same(iota((rank, width), 1) & (rank - 1), iota((rank, width), 0))
        for c in range(start, start + size):
            tiled = mm(coup[c].reshape(wide, rank), tile)
            picks = same(quo(iota((width, far), 0), rank) + start, place[c : c + 1, :])
            chosen = nt(spread_rows, picks)
            rmat[c, :, :width] = (tiled * chosen).astype(BF16)
    up_wide = [mm(up, tile_wide) for up in ups]

    def couple(number, carry):
        base = number * chunk
        sums = []
        for start, size in levels:
            total = None
            for c in range(start, start + size):
                mine = same(quo(iota((chunk * own, far), 0), own) + base, owner[c : c + 1, :])
                left = mm(mine, spread_k) * jnp.concatenate([up_wide[c]] * chunk, axis=0)
                term = mm(left.astype(BF16), rmat[c, :, : size * rank])
                total = term if total is None else total + term
            sums.append(total)
        spare = fsend.shape[2] - clusters * rank
        if spare:
            sums.append(jnp.zeros((chunk * own, spare), F32))
        joined = jnp.concatenate(sums, axis=1).astype(BF16)
        fsend[pl.ds(base, chunk)] = joined.reshape(chunk, own, fsend.shape[2])
        return carry

    lax.fori_loop(0, trees // chunk, couple, 0, unroll=trees == chunk)

    def far_copy(step):
        to = lax.rem(tree + step, jnp.int32(trees))
        return pltpu.make_async_remote_copy(
            src_ref=fsend.at[to],
            dst_ref=frecv.at[tree],
            send_sem=f_send.at[to],
            recv_sem=f_recv.at[tree],
            device_id=(to, sub),
            device_id_type=MESH,
        )

    def far_arrived(step):
        source = lax.rem(tree + step, jnp.int32(trees))
        pltpu.make_async_remote_copy(
            src_ref=fsend.at[source],
            dst_ref=frecv.at[source],
            send_sem=f_send.at[source],
            recv_sem=f_recv.at[source],
            device_id=(source, sub),
            device_id_type=MESH,
        ).wait_recv()
        return source

    def start_far(step, carry):
        far_copy(step).start()
        return carry

    heard = (tree >= half).astype(jnp.int32) + (tree + half < trees).astype(jnp.int32)
    pl.semaphore_wait(known, heard)
    lax.fori_loop(1, trees, start_far, 0, unroll=trees <= 16)

    rows = groups * own
    totals = [jnp.zeros((rows, leaf), F32)] * pair
    for slot in (1, 0, 2):
        for step in range(groups):
            if (slot, step) != (1, 0):
                guarded(has[slot], functools.partial(arrived, slot, step))
        piece = win[slot].reshape(rows, subtree * leaf)
        for core_step in range(pair):
            if core_step > 0:
                swap(core_step, slot).wait_recv()
            held = wown if core_step == 0 else wpeer.at[core_step - 1]
            blocks = held[slot * subtree : (slot + 1) * subtree].reshape(subtree * leaf, leaf)
            totals[core_step] = totals[core_step] + mm(piece, blocks)

    for core_step in range(pair):
        leaf_core = lax.rem(core + core_step, jnp.int32(pair))
        nsend[:, leaf_core] = totals[core_step].reshape(groups, own, leaf).astype(BF16)
    nrecv[group] = nsend[group]

    def near_copy(step):
        to = lax.rem(group + step, jnp.int32(groups))
        return pltpu.make_async_remote_copy(
            src_ref=nsend.at[to],
            dst_ref=nrecv.at[group],
            send_sem=n_send.at[to],
            recv_sem=n_recv.at[group],
            device_id=(tree, other(step)),
            device_id_type=MESH,
        )

    def near_arrived(step):
        source = lax.rem(group + step, jnp.int32(groups))
        pltpu.make_async_remote_copy(
            src_ref=nsend.at[source],
            dst_ref=nrecv.at[source],
            send_sem=n_send.at[source],
            recv_sem=n_recv.at[source],
            device_id=(tree, other(step)),
            device_id_type=MESH,
        ).wait_recv()

    for step in range(1, groups):
        near_copy(step).start()

    def add_far(step, carry):
        return carry + frecv[far_arrived(step)].astype(F32)

    incoming = lax.fori_loop(1, trees, add_far, fsend[tree].astype(F32), unroll=trees <= 16)
    far_part = mm(incoming.astype(BF16), dmat[...])

    for step in range(1, groups):
        near_arrived(step)
    for s in range(subtree):
        near_part = nrecv[s // pair, s % pair].astype(F32)
        out_ref[:, s * leaf : (s + 1) * leaf] = (near_part + far_part[:, s * leaf : (s + 1) * leaf]).astype(BF16)

    for slot, step in first_hops:
        guarded(goes[slot], functools.partial(lambda a, b: spread(a, b).wait_send(), slot, step))
    for core_step in range(1, pair):
        for slot in range(3):
            swap(core_step, slot).wait_send()

    def end_far(step, carry):
        far_copy(step).wait_send()
        return carry

    lax.fori_loop(1, trees, end_far, 0, unroll=trees <= 16)
    for step in range(1, groups):
        near_copy(step).wait_send()


def local(vectors, near_blocks, near_cols, near_mask, leaf_basis, transfer, coupling, far_targets, far_mask):
    trees, subs = lax.axis_size("leaf"), lax.axis_size("sub")
    pair = 2 if subs % 2 == 0 else 1
    groups = subs // pair
    chunk = 8 if trees % 8 == 0 else trees
    own, points = vectors.shape
    clusters, far, rank = coupling.shape[:3]
    leaf = leaf_basis.shape[2]
    window = 3 * leaf_basis.shape[0]
    lanes = -(-clusters * rank // 128) * 128
    any_spec = pl.BlockSpec(memory_space=pl.ANY)
    smem = pl.BlockSpec(memory_space=pltpu.SMEM)
    dma = pltpu.SemaphoreType.DMA
    return pl.pallas_call(
        functools.partial(kernel, (trees, subs, pair, chunk)),
        out_shape=jax.ShapeDtypeStruct((own, points), BF16),
        in_specs=[any_spec, any_spec, smem, smem] + [any_spec] * 5,
        out_specs=pl.BlockSpec(memory_space=pltpu.VMEM),
        scratch_shapes=[
            pltpu.VMEM((3, groups, own, points), BF16),
            pltpu.VMEM(near_blocks.shape[1:], BF16),
            pltpu.VMEM((window, leaf, leaf), BF16),
            pltpu.VMEM((max(1, pair - 1), window, leaf, leaf), BF16),
            pltpu.VMEM(leaf_basis.shape, BF16),
            pltpu.VMEM(transfer.shape, BF16),
            pltpu.VMEM(coupling.shape, BF16),
            pltpu.VMEM(far_targets.shape, jnp.int32),
            pltpu.VMEM(far_mask.shape, jnp.int32),
            pltpu.VMEM((lanes, points), BF16),
            pltpu.VMEM((clusters, far * rank, leaf_basis.shape[0] * rank), BF16),
            pltpu.VMEM((trees, own, lanes), BF16),
            pltpu.VMEM((trees, own, lanes), BF16),
            pltpu.VMEM((groups, pair, own, leaf), BF16),
            pltpu.VMEM((groups, pair, own, leaf), BF16),
            pltpu.SemaphoreType.REGULAR,
            dma((7,)),
            dma((3, groups)),
            dma((3, groups)),
            dma((max(1, pair - 1), 3)),
            dma((max(1, pair - 1), 3)),
            dma((trees,)),
            dma((trees,)),
            dma((groups,)),
            dma((groups,)),
        ],
        compiler_params=pltpu.CompilerParams(collective_id=0, has_side_effects=True),
    )(vectors, near_blocks, near_cols, near_mask, leaf_basis, transfer, coupling, far_targets, far_mask)


def solution(mesh):
    return jax.shard_map(
        local,
        mesh=mesh,
        in_specs=(
            P("sub", "leaf"),
            P(("leaf", "sub"), None, None, None),
            P(("leaf", "sub"), None),
            P(("leaf", "sub"), None),
            P("leaf", None, None),
            P("leaf", None, None),
            P("leaf", None, None, None),
            P("leaf", None),
            P("leaf", None),
        ),
        out_specs=P("sub", "leaf"),
        check_vma=False,
    )
```
